512 devices in a mesh: strip: 32 (over z, core), front: 16 (over y, x).
Axes of the slice: x: 4, y: 4, z: 16, core: 2. Of those that a mesh axis runs over, the one named last changes fastest.
Arguments:
- topmost_facet_vertex_table: int32 [32, 1024, 3], P('strip', 'front'), may hold values from 0 to 2047, as said below
- neighbour_bottom_vertex_table: int32 [32, 1024, 3], P('strip', 'front'), may hold values from 0 to 2047, as said below
- topmost_facet_forcing: bfloat16 [32, 1024, 6, 128], P('strip', 'front'), may hold values from -6 to 6
- bottom_facet_forcing: bfloat16 [32, 1024, 6, 128], P('strip', 'front'), may hold values from -6 to 6
- interior_unknown_forcing: bfloat16 [32, 1024, 128], P('strip', 'front'), may hold values from -6 to 6
- interior_elimination_matrix: bfloat16 [32, 1024, 4096], P('strip', 'front'), may hold values from -0.1875 to 0.1875
- border_interaction_matrix: bfloat16 [32, 4096, 4096], P('strip', None, 'front'), may hold values from -0.0625 to 0.0625
- reciprocal_diagonal_factor: bfloat16 [32, 4096, 4096], P('strip', 'front'), may hold values from -0.2 to 1.5
- initial_received_border: bfloat16 [32, 32, 4096], P('strip', None, 'front'), may hold values from -6 to 6
Outputs:
- fronts: bfloat16 [32, 4, 32, 4096], P('strip', None, None, 'front')
The draws below stay inside these ranges and needn't reach their ends.
Inputs may be any that keep to these rules, and one draw needn't show every extreme that they name: `topmost_facet_vertex_table`: row e of a strip lists the node numbers of the three edge nodes of element e (corner, midside, corner), in that front's own node order, with 2048 nodes on a front. `neighbour_bottom_vertex_table`: row e of strip s lists the three edge nodes of element e of strip s + 1's bottom row, in strip s's front node order.
All inputs are finite; a program needn't handle non-finite values.
Results may differ from the reference program's by a relative error of at most 0.0075.
Values may be sent and summed in bfloat16 or wider, within the bound.
A program may use at most 64 MiB of HBM per device.

```python
import jax
import jax.numpy as jnp
from jax import lax

RANK_UNKNOWNS = 4096
SCENARIO_GROUP = 32
STEPS = 4
NI = 1024
NODES = 2048
ELEMS = 1024
GRID_LAYERS = 32
CASES = 128


def node_rows(key, salt):
    keys = jax.random.split(jax.random.fold_in(key, salt), GRID_LAYERS)
    places = (2 * jnp.arange(ELEMS, dtype=jnp.int32)[:, None] + jnp.arange(3, dtype=jnp.int32)[None, :]) % NODES

    def single(one_key):
        ordering = jax.random.permutation(one_key, NODES).astype(jnp.int32)
        return ordering[places]
    return jax.vmap(single)(keys)


def draw_topmost_facet_vertex_table(key, part):
    return node_rows(key, 11)


def draw_neighbour_bottom_vertex_table(key, part):
    return node_rows(key, 23)


def draw_reciprocal_diagonal_factor(key, part):
    first_key, second_key = jax.random.split(jax.random.fold_in(key, 37))
    diagonal = jax.random.uniform(first_key, (GRID_LAYERS, RANK_UNKNOWNS), jnp.float32, 0.7, 1.3)
    noise = jax.random.truncated_normal(second_key, -3.0, 3.0, (GRID_LAYERS, RANK_UNKNOWNS, RANK_UNKNOWNS), jnp.float32)
    noise = noise * (0.5 / RANK_UNKNOWNS ** 0.5)
    identity = jnp.eye(RANK_UNKNOWNS, dtype=jnp.float32)
    return (noise + diagonal[:, :, None] * identity[None, :, :]).astype(jnp.bfloat16)


def steps_of(stream_key, dims, shards, smallest, top_value):
    gain = 1.0
    for axis_at, shards_of in shards:
        heights = jax.random.uniform(jax.random.fold_in(jax.random.fold_in(stream_key, 6), axis_at), (shards_of,), jnp.float32, smallest / len(shards), top_value / len(shards))
        gain = gain * jnp.repeat(jnp.exp(heights), dims[axis_at] // shards_of).reshape((-1,) + (1,) * (len(dims) - 1 - axis_at))
    return gain


def normal_values(key, extent, deviation, most, cuts=(), kind=jnp.bfloat16):
    gain = steps_of(key, extent, cuts, -0.22, 0.18) if cuts else 1.0
    values = jax.random.normal(key, extent, jnp.float32) * deviation * gain
    return jnp.minimum(jnp.maximum(values, -most), most).astype(kind)


def setup_inputs(seed: int = 0) -> dict:
    arg_keys = jax.random.split(jax.random.key(seed), 10)
    topmost_facet_vertex_table = draw_topmost_facet_vertex_table(jax.random.fold_in(arg_keys[9], 71), 0)
    neighbour_bottom_vertex_table = draw_neighbour_bottom_vertex_table(jax.random.fold_in(arg_keys[9], 71), 0)
    topmost_facet_forcing = normal_values(arg_keys[2], (GRID_LAYERS, ELEMS, 6, CASES), 1.0, 6.0, ((0, 32), (1, 16)))
    bottom_facet_forcing = normal_values(arg_keys[3], (GRID_LAYERS, ELEMS, 6, CASES), 1.0, 6.0, ((0, 32), (1, 16)))
    interior_unknown_forcing = normal_values(arg_keys[4], (GRID_LAYERS, NI, CASES), 1.0, 6.0, ((0, 32), (1, 16)))
    interior_elimination_matrix = normal_values(arg_keys[5], (GRID_LAYERS, NI, RANK_UNKNOWNS), NI ** -0.5, 0.1875, ((0, 32), (1, 16)))
    border_interaction_matrix = normal_values(arg_keys[6], (GRID_LAYERS, RANK_UNKNOWNS, RANK_UNKNOWNS), (2 * RANK_UNKNOWNS) ** -0.5, 0.0625, ((0, 32), (2, 16)))
    reciprocal_diagonal_factor = draw_reciprocal_diagonal_factor(jax.random.fold_in(arg_keys[9], 71), 0)
    initial_received_border = normal_values(arg_keys[8], (GRID_LAYERS, SCENARIO_GROUP, RANK_UNKNOWNS), 1.0, 6.0, ((0, 32), (2, 16)))
    return dict(topmost_facet_vertex_table=topmost_facet_vertex_table, neighbour_bottom_vertex_table=neighbour_bottom_vertex_table, topmost_facet_forcing=topmost_facet_forcing, bottom_facet_forcing=bottom_facet_forcing, interior_unknown_forcing=interior_unknown_forcing, interior_elimination_matrix=interior_elimination_matrix, border_interaction_matrix=border_interaction_matrix, reciprocal_diagonal_factor=reciprocal_diagonal_factor, initial_received_border=initial_received_border)


def incidence_sum(node_ids, edge_loads):
    dof_ids = (2 * node_ids[:, :, None] + jnp.arange(2, dtype=jnp.int32)[None, None, :]).reshape(-1)
    table = (jnp.arange(RANK_UNKNOWNS, dtype=jnp.int32)[:, None] == dof_ids[None, :]).astype(jnp.bfloat16)
    flat = edge_loads.reshape(-1, edge_loads.shape[-1])
    return jnp.dot(table, flat, preferred_element_type=jnp.float32)


def strip_assembly(pieces):
    own_nodes, lower_nodes, own_loads, upper_loads, inner_loads, condense_map = pieces
    assembled = incidence_sum(own_nodes, own_loads) + incidence_sum(lower_nodes, upper_loads)
    return assembled - jnp.dot(condense_map.T, inner_loads, preferred_element_type=jnp.float32)


def advance(pieces):
    received_border_vector, case_loads, couple_map, inverse_map = pieces
    reduced = (case_loads - jnp.dot(received_border_vector, couple_map, preferred_element_type=jnp.float32)).astype(jnp.bfloat16)
    return jnp.dot(reduced, inverse_map, preferred_element_type=jnp.float32).astype(jnp.bfloat16)


def reference(topmost_facet_vertex_table, neighbour_bottom_vertex_table, topmost_facet_forcing, bottom_facet_forcing, interior_unknown_forcing, interior_elimination_matrix, border_interaction_matrix, reciprocal_diagonal_factor, initial_received_border):
    upper_loads = jnp.concatenate([bottom_facet_forcing[1:], jnp.zeros_like(bottom_facet_forcing[:1])], 0)
    front_loads = lax.map(strip_assembly, (topmost_facet_vertex_table, neighbour_bottom_vertex_table, topmost_facet_forcing, upper_loads, interior_unknown_forcing, interior_elimination_matrix))
    received_border_vector = initial_received_border
    results = []
    for window_step in range(STEPS):
        case_loads = jnp.swapaxes(front_loads[:, :, window_step * SCENARIO_GROUP:(window_step + 1) * SCENARIO_GROUP], 1, 2)
        outgoing = lax.map(advance, (received_border_vector, case_loads, border_interaction_matrix, reciprocal_diagonal_factor))
        results.append(outgoing)
        received_border_vector = jnp.concatenate([jnp.zeros_like(outgoing[:1]), outgoing[:-1]], 0)
    return jnp.stack(results, 1)
```

```python
import functools

import jax
import jax.numpy as jnp
from jax import lax
from jax.experimental import pallas as pl
from jax.experimental.pallas import tpu as pltpu
from jax.sharding import PartitionSpec as P

MESH = pl.DeviceIdType.MESH
STEPS = 4
SIDE = 4
F32, BF16 = jnp.float32, jnp.bfloat16


def ring_gap(step):
    return min(step, SIDE - step)


def reach(k):
    return ring_gap(k // SIDE) + ring_gap(k % SIDE)


def kernel(
    strips,
    fronts,
    own_table,
    low_table,
    top_loads,
    bottom_loads,
    inner_loads,
    condense,
    couple_hbm,
    inverse_hbm,
    first_front,
    out,
    couple,
    inverse,
    own_nodes,
    low_nodes,
    upper,
    lhs_own,
    lhs_up,
    partial,
    load_send,
    load_own,
    load_slots,
    front_slots,
    sum_send,
    sum_slots,
    weight_sem,
    upper_sems,
    load_sems,
    load_send_sems,
    front_sems,
    front_send_sems,
    sum_sems,
    sum_send_sems,
):
    strip, front = lax.axis_index("strip"), lax.axis_index("front")
    row, col = front // SIDE, front % SIDE
    group, width = first_front.shape
    cases = inner_loads.shape[1]
    far_first = sorted(range(1, fronts), key=lambda k: -reach(k))
    near_first = sorted(range(1, fronts), key=reach)

    def ahead(k):
        return ((row + k // SIDE) % SIDE) * SIDE + (col + k % SIDE) % SIDE

    def behind(k):
        return ((row + SIDE - k // SIDE) % SIDE) * SIDE + (col + SIDE - k % SIDE) % SIDE

    def send(src, dst, send_sem, recv_sem, where):
        return pltpu.make_async_remote_copy(
            src_ref=src,
            dst_ref=dst,
            send_sem=send_sem,
            recv_sem=recv_sem,
            device_id=where,
            device_id_type=MESH,
        )

    def landed(ref, sem):
        pltpu.make_async_copy(ref, ref, sem).wait()

    load_weights = [
        pltpu.make_async_copy(couple_hbm, couple, weight_sem.at[0]),
        pltpu.make_async_copy(inverse_hbm, inverse, weight_sem.at[1]),
    ]
    for copy in load_weights:
        copy.start()

    barrier = pltpu.get_barrier_semaphore()
    for k in near_first:
        pl.semaphore_signal(barrier, 1, device_id=(strip, ahead(k)), device_id_type=MESH)

    @pl.when(strip < strips - 1)
    def _():
        pl.semaphore_signal(barrier, 1, device_id=(strip + 1, front), device_id_type=MESH)

    @pl.when(strip > 0)
    def _():
        pl.semaphore_signal(barrier, 1, device_id=(strip - 1, front), device_id_type=MESH)

    def incidence(table, columns):
        start = columns * width
        dofs = lax.broadcasted_iota(jnp.int32, (table.shape[0], width), 1) + start
        tiles = []
        for j in range(6):
            ids = 2 * table[:, j // 2 : j // 2 + 1] + j % 2
            tiles.append(jnp.where(dofs == ids, 1.0, 0.0).astype(BF16))
        return jnp.concatenate(tiles, axis=0)

    def turned(loads):
        return loads[...].reshape(-1, cases).astype(F32).T

    edge_rows = 6 * top_loads.shape[1]
    own_nodes[...] = own_table[:, 0].T
    low_nodes[...] = low_table[:, 0].T
    lhs_own[:, :edge_rows] = turned(top_loads).astype(BF16)
    lhs_own[:, edge_rows:] = (-inner_loads[...].astype(F32).T).astype(BF16)

    @pl.loop(0, fronts)
    def _(k):
        where = ahead(k)
        at = pl.ds(pl.multiple_of(where * width, width), width)
        rhs = jnp.concatenate([incidence(own_nodes, where), condense[:, at]], axis=0)
        partial[k] = jnp.dot(lhs_own[...], rhs, preferred_element_type=F32)

    below = jnp.minimum(strip, 1)
    above = jnp.minimum(strips - 1 - strip, 1)
    pl.semaphore_wait(barrier, fronts - 1 + below + above)

    @pl.when(strip > 0)
    def _():
        send(bottom_loads, upper, upper_sems.at[0], upper_sems.at[1], (strip - 1, front)).start()

    for k in far_first:
        send(
            first_front,
            front_slots.at[0, k],
            front_send_sems.at[0],
            front_sems.at[0, k],
            (strip, ahead(k)),
        ).start()
    front_slots[0, 0] = first_front[...]

    @pl.when(strip == 0)
    def _():
        for step in range(1, STEPS):
            front_slots[step] = jnp.zeros_like(front_slots[step])

    @pl.when(strip == strips - 1)
    def _():
        upper[...] = jnp.zeros_like(upper)

    @pl.when(strip < strips - 1)
    def _():
        landed(upper, upper_sems.at[1])

    lhs_up[...] = turned(upper).astype(BF16)

    def load_copy(step, k, where):
        return send(
            load_send.at[k, step],
            load_slots.at[step, k],
            load_send_sems.at[step],
            load_sems.at[step, k],
            (strip, where),
        )

    @pl.loop(0, fronts - 1)
    def _(i):
        k = (i + 10) % (fronts - 1) + 1
        where = ahead(k)
        both = partial[k] + jnp.dot(
            lhs_up[...], incidence(low_nodes, where), preferred_element_type=F32
        )
        load_send[k] = both.astype(BF16).reshape(STEPS, group, width)
        load_copy(0, k, where).start()

    both = partial[0] + jnp.dot(lhs_up[...], incidence(low_nodes, front), preferred_element_type=F32)
    load_own[...] = both.reshape(STEPS, group, width)

    for copy in load_weights:
        copy.wait()

    @pl.loop(0, STEPS)
    def _(step):
        joined = jnp.zeros((group, width), F32)
        for k in [0, *near_first]:
            if k == 0:
                expected = (step > 0) & (strip > 0)
            else:
                expected = (step == 0) | (strip > 0)

            @pl.when(expected)
            def _():
                landed(front_slots.at[step, k], front_sems.at[step, k])

            at = pl.ds(pl.multiple_of(behind(k) * width, width), width)
            joined = joined + jnp.dot(
                front_slots[step, k], couple[at, :], preferred_element_type=F32
            )

        total = load_own[step]
        for k in near_first:
            landed(load_slots.at[step, k], load_sems.at[step, k])
            total = total + load_slots[step, k].astype(F32)
        reduced = (total - joined).astype(BF16)

        for k in far_first:
            where = ahead(k)
            at = pl.ds(pl.multiple_of(where * width, width), width)
            sum_send[step, k] = jnp.dot(
                reduced, inverse[:, at], preferred_element_type=F32
            ).astype(BF16)
            send(
                sum_send.at[step, k],
                sum_slots.at[step, k],
                sum_send_sems.at[step],
                sum_sems.at[step, k],
                (strip, where),
            ).start()

        @pl.when(step < STEPS - 1)
        def _():
            for k in far_first:
                load_copy(step + 1, k, ahead(k)).start()

        at = pl.ds(pl.multiple_of(front * width, width), width)
        summed = jnp.dot(reduced, inverse[:, at], preferred_element_type=F32)
        for k in near_first:
            landed(sum_slots.at[step, k], sum_sems.at[step, k])
            summed = summed + sum_slots[step, k].astype(F32)
        out[step] = summed.astype(BF16)

        @pl.when((step < STEPS - 1) & (strip < strips - 1))
        def _():
            for k in [*far_first, 0]:
                send(
                    out.at[step],
                    front_slots.at[step + 1, k],
                    front_send_sems.at[step + 1],
                    front_sems.at[step + 1, k],
                    (strip + 1, ahead(k)),
                ).start()

    @pl.when(strip > 0)
    def _():
        landed(upper, upper_sems.at[0])

    landed(front_slots.at[0, pl.ds(1, fronts - 1)], front_send_sems.at[0])
    for step in range(STEPS):
        landed(sum_slots.at[step, pl.ds(1, fronts - 1)], sum_send_sems.at[step])
        landed(load_slots.at[step, pl.ds(1, fronts - 1)], load_send_sems.at[step])

    @pl.when(strip < strips - 1)
    def _():
        for step in range(1, STEPS):
            landed(front_slots.at[step], front_send_sems.at[step])


def solution(mesh):
    strips, fronts = mesh.shape["strip"], mesh.shape["front"]

    def shards(*blocks):
        tables = [jnp.transpose(block, (2, 0, 1)) for block in blocks[:2]]
        blocks = tables + [block[0] for block in blocks[2:]]
        for i in (2, 3):
            blocks[i] = jnp.swapaxes(blocks[i], 0, 1)
        elements = blocks[2].shape[1]
        inner, cases = blocks[4].shape
        dofs, width = blocks[6].shape
        group = blocks[8].shape[0]
        in_vmem = pl.BlockSpec(memory_space=pltpu.VMEM)
        in_hbm = pl.BlockSpec(memory_space=pl.ANY)
        slots = pltpu.VMEM((STEPS, fronts, group, width), BF16)
        dma = pltpu.SemaphoreType.DMA
        result = pl.pallas_call(
            functools.partial(kernel, strips, fronts),
            out_shape=jax.ShapeDtypeStruct((STEPS, group, width), BF16),
            in_specs=[in_vmem] * 6 + [in_hbm] * 2 + [in_vmem],
            out_specs=in_vmem,
            scratch_shapes=[
                pltpu.VMEM((dofs, width), BF16),
                pltpu.VMEM((width, dofs), BF16),
                pltpu.VMEM((elements, 3), jnp.int32),
                pltpu.VMEM((elements, 3), jnp.int32),
                pltpu.VMEM((6, elements, cases), BF16),
                pltpu.VMEM((cases, 6 * elements + inner), BF16),
                pltpu.VMEM((cases, 6 * elements), BF16),
                pltpu.VMEM((fronts, cases, width), F32),
                pltpu.VMEM((fronts, STEPS, group, width), BF16),
                pltpu.VMEM((STEPS, group, width), F32),
                slots,
                slots,
                slots,
                slots,
                dma((2,)),
                dma((2,)),
                dma((STEPS, fronts)),
                dma((STEPS,)),
                dma((STEPS, fronts)),
                dma((STEPS,)),
                dma((STEPS, fronts)),
                dma((STEPS,)),
            ],
            compiler_params=pltpu.CompilerParams(collective_id=0, has_side_effects=True),
        )(*blocks)
        return result[None]

    return jax.shard_map(
        shards,
        mesh=mesh,
        in_specs=(
            P("strip", "front", None),
            P("strip", "front", None),
            P("strip", "front", None, None),
            P("strip", "front", None, None),
            P("strip", "front", None),
            P("strip", "front", None),
            P("strip", None, "front"),
            P("strip", "front", None),
            P("strip", None, "front"),
        ),
        out_specs=P("strip", None, None, "front"),
        check_vma=False,
    )
```

```python
import functools

import jax
import jax.numpy as jnp
from jax import lax
from jax.experimental import pallas as pl
from jax.experimental.pallas import tpu as pltpu
from jax.sharding import PartitionSpec as P

MESH = pl.DeviceIdType.MESH
STEPS = 4
SIDE = 4
F32, BF16 = jnp.float32, jnp.bfloat16


def ring_gap(step):
    return min(step, SIDE - step)


def reach(k):
    return ring_gap(k // SIDE) + ring_gap(k % SIDE)


def kernel(
    strips,
    fronts,
    own_table_hbm,
    low_table_hbm,
    top_hbm,
    bottom_hbm,
    inner_hbm,
    condense_hbm,
    couple_hbm,
    inverse_hbm,
    first_hbm,
    out,
    own_table,
    low_table,
    top_loads,
    bottom_loads,
    inner_loads,
    condense,
    couple,
    inverse,
    first_front,
    own_nodes,
    low_nodes,
    upper,
    lhs_own,
    lhs_up,
    low_marks,
    partial,
    load_send,
    load_own,
    load_slots,
    front_slots,
    sum_send,
    sum_slots,
    input_sems,
    upper_sems,
    load_sems,
    tile_sems,
    near_sems,
    far_sems,
    sum_sems,
    send_sems,
):
    strip, front = lax.axis_index("strip"), lax.axis_index("front")
    row, col = front // SIDE, front % SIDE
    group, width = first_front.shape
    cases = inner_loads.shape[1]
    peers = sorted(range(1, fronts), key=lambda k: -reach(k))
    far = [k for k in peers if reach(k) > 2]
    near = [k for k in peers if reach(k) <= 2]
    batches = [far, near[: len(near) // 2], near[len(near) // 2 :]]
    across = strip % 2

    def ahead(k):
        return ((row + k // SIDE) % SIDE) * SIDE + (col + k % SIDE) % SIDE

    def behind(k):
        return ((row + SIDE - k // SIDE) % SIDE) * SIDE + (col + SIDE - k % SIDE) % SIDE

    def panel(where):
        return pl.ds(pl.multiple_of(where * width, width), width)

    def send(src, dst, send_sem, recv_sem, where):
        pltpu.make_async_remote_copy(
            src_ref=src,
            dst_ref=dst,
            send_sem=send_sem,
            recv_sem=recv_sem,
            device_id=where,
            device_id_type=MESH,
        ).start()

    def landed(ref, sem):
        pltpu.make_async_copy(ref, ref, sem).wait()

    barrier = pltpu.get_barrier_semaphore()
    for k in peers:
        pl.semaphore_signal(barrier, 1, device_id=(strip, ahead(k)), device_id_type=MESH)

    @pl.when(strip < strips - 1)
    def _():
        pl.semaphore_signal(barrier, 1, device_id=(strip + 1, front), device_id_type=MESH)

    @pl.when(strip > 0)
    def _():
        pl.semaphore_signal(barrier, 1, device_id=(strip - 1, front), device_id_type=MESH)

    fetches = [
        pltpu.make_async_copy(src, dst, input_sems.at[i])
        for i, (src, dst) in enumerate(
            [
                (own_table_hbm, own_table),
                (top_hbm, top_loads),
                (inner_hbm, inner_loads),
                (condense_hbm, condense),
                (bottom_hbm, bottom_loads),
                (first_hbm, first_front),
                (low_table_hbm, low_table),
                (couple_hbm, couple),
                (inverse_hbm, inverse),
            ]
        )
    ]
    for copy in fetches:
        copy.start()

    def incidence(table, columns):
        dofs = lax.broadcasted_iota(jnp.int32, (table.shape[0], width), 1) + columns * width
        tiles = []
        for j in range(6):
            ids = 2 * table[:, j // 2 : j // 2 + 1] + j % 2
            tiles.append(jnp.where(dofs == ids, 1.0, 0.0).astype(BF16))
        return jnp.concatenate(tiles, axis=0)

    def turned(loads):
        return loads[...].reshape(-1, cases).astype(F32).T

    edge_rows = 6 * top_loads.shape[1]
    for copy in fetches[:4]:
        copy.wait()
    own_nodes[...] = own_table[:, 0].T
    lhs_own[:, :edge_rows] = turned(top_loads).astype(BF16)
    lhs_own[:, edge_rows:] = (-inner_loads[...].astype(F32).T).astype(BF16)

    @pl.loop(0, fronts)
    def _(k):
        where = ahead(k)
        rhs = jnp.concatenate([incidence(own_nodes, where), condense[:, panel(where)]], axis=0)
        partial[k] = jnp.dot(lhs_own[...], rhs, preferred_element_type=F32)

    for copy in fetches[4:7]:
        copy.wait()

    below = jnp.minimum(strip, 1)
    above = jnp.minimum(strips - 1 - strip, 1)
    pl.semaphore_wait(barrier, fronts - 1 + below + above)

    @pl.when(strip > 0)
    def _():
        send(bottom_loads, upper, upper_sems.at[0], upper_sems.at[1], (strip - 1, front))

    def gather_sem(step, k):
        return (near_sems if k in near else far_sems).at[step]

    for k in peers:
        send(
            first_front,
            front_slots.at[0, k],
            send_sems.at[0],
            gather_sem(0, k),
            (strip, ahead(k)),
        )
    front_slots[0, 0] = first_front[...]

    @pl.when(strip == 0)
    def _():
        for step in range(1, STEPS):
            front_slots[step] = jnp.zeros_like(front_slots[step])

    @pl.when(strip == strips - 1)
    def _():
        upper[...] = jnp.zeros_like(upper)

    low_nodes[...] = low_table[:, 0].T

    @pl.loop(0, fronts)
    def _(k):
        low_marks[k] = incidence(low_nodes, ahead(k))

    @pl.when(strip < strips - 1)
    def _():
        landed(upper, upper_sems.at[1])

    lhs_up[...] = turned(upper).astype(BF16)

    def loads_of(k, rows):
        return partial[k, rows] + jnp.dot(lhs_up[rows], low_marks[k], preferred_element_type=F32)

    def send_loads(step, ks):
        for k in ks:
            send(
                load_send.at[step, k],
                load_slots.at[step, k],
                send_sems.at[1],
                load_sems.at[step],
                (strip, ahead(k)),
            )

    for batch in batches:
        for k in batch:
            load_send[0, k] = loads_of(k, slice(0, group)).astype(BF16)
        send_loads(0, batch)
    load_own[0] = loads_of(0, slice(0, group))

    @pl.loop(0, fronts)
    def _(k):
        rest = loads_of(k, slice(group, cases)).astype(BF16)
        for step in range(1, STEPS):
            load_send[step, k] = rest[(step - 1) * group : step * group]

    rest = loads_of(0, slice(group, cases))
    for step in range(1, STEPS):
        load_own[step] = rest[(step - 1) * group : step * group]

    for copy in fetches[7:]:
        copy.wait()

    @pl.loop(0, STEPS)
    def _(step):
        @pl.when((step > 0) & (strip > 0))
        def _():
            landed(front_slots.at[step, 0], tile_sems.at[step])

        @pl.when((step > 0) & (strip > 0) & (across == 0))
        def _():
            for k in peers:
                send(
                    front_slots.at[step, 0],
                    front_slots.at[step, k],
                    send_sems.at[2],
                    gather_sem(step, k),
                    (strip, ahead(k)),
                )

        def joined_with(ks):
            return functools.reduce(
                jnp.add,
                [
                    jnp.dot(
                        front_slots[step, k],
                        couple[panel(behind(k)), :],
                        preferred_element_type=F32,
                    )
                    for k in ks
                ],
            )

        expected = (step == 0) | (strip > 0)

        @pl.when(expected)
        def _():
            landed(front_slots.at[step, pl.ds(0, len(near))], near_sems.at[step])

        joined = joined_with([0, *near])

        @pl.when(expected)
        def _():
            landed(front_slots.at[step, pl.ds(0, len(far))], far_sems.at[step])

        joined = joined + joined_with(far)

        landed(load_slots.at[step, pl.ds(1, fronts - 1)], load_sems.at[step])
        total = load_own[step]
        for k in peers:
            total = total + load_slots[step, k].astype(F32)
        reduced = (total - joined).astype(BF16)

        def sums_for(where):
            return jnp.dot(reduced, inverse[:, panel(where)], preferred_element_type=F32)

        for batch in batches:
            for k in batch:
                sum_send[step, k] = sums_for(ahead(k)).astype(BF16)
            for k in batch:
                send(
                    sum_send.at[step, k],
                    sum_slots.at[step, k],
                    send_sems.at[3],
                    sum_sems.at[step],
                    (strip, ahead(k)),
                )
        summed = sums_for(front)

        @pl.when(step < STEPS - 1)
        def _():
            send_loads(step + 1, peers)

        landed(sum_slots.at[step, pl.ds(1, fronts - 1)], sum_sems.at[step])
        for k in peers:
            summed = summed + sum_slots[step, k].astype(F32)
        out[step] = summed.astype(BF16)

        onward = (step < STEPS - 1) & (strip < strips - 1)

        @pl.when(onward & (across == 0))
        def _():
            for k in [*far, *near, 0]:
                send(
                    out.at[step],
                    front_slots.at[step + 1, k],
                    send_sems.at[4],
                    tile_sems.at[step + 1] if k == 0 else gather_sem(step + 1, k),
                    (strip + 1, ahead(k)),
                )

        @pl.when(onward & (across == 1))
        def _():
            send(
                out.at[step],
                front_slots.at[step + 1, 0],
                send_sems.at[4],
                tile_sems.at[step + 1],
                (strip + 1, front),
            )

    @pl.when(strip > 0)
    def _():
        landed(upper, upper_sems.at[0])

    others = pl.ds(1, fronts - 1)
    landed(front_slots.at[0, others], send_sems.at[0])
    landed(load_slots.at[:, others], send_sems.at[1])
    landed(sum_slots.at[:, others], send_sems.at[3])

    @pl.when((strip > 0) & (across == 0))
    def _():
        landed(front_slots.at[pl.ds(1, STEPS - 1), others], send_sems.at[2])

    @pl.when((strip < strips - 1) & (across == 0))
    def _():
        landed(front_slots.at[pl.ds(1, STEPS - 1)], send_sems.at[4])

    @pl.when((strip < strips - 1) & (across == 1))
    def _():
        landed(front_slots.at[pl.ds(1, STEPS - 1), 0], send_sems.at[4])


def solution(mesh):
    strips, fronts = mesh.shape["strip"], mesh.shape["front"]

    def shards(*blocks):
        tables = [jnp.transpose(block, (2, 0, 1)) for block in blocks[:2]]
        blocks = tables + [block[0] for block in blocks[2:]]
        for i in (2, 3):
            blocks[i] = jnp.swapaxes(blocks[i], 0, 1)
        elements = blocks[2].shape[1]
        inner, cases = blocks[4].shape
        group, width = blocks[8].shape
        in_vmem = pl.BlockSpec(memory_space=pltpu.VMEM)
        in_hbm = pl.BlockSpec(memory_space=pl.ANY)
        slots = pltpu.VMEM((STEPS, fronts, group, width), BF16)
        dma = pltpu.SemaphoreType.DMA
        result = pl.pallas_call(
            functools.partial(kernel, strips, fronts),
            out_shape=jax.ShapeDtypeStruct((STEPS, group, width), BF16),
            in_specs=[in_hbm] * len(blocks),
            out_specs=in_vmem,
            scratch_shapes=[
                *[pltpu.VMEM(block.shape, block.dtype) for block in blocks],
                pltpu.VMEM((elements, 3), jnp.int32),
                pltpu.VMEM((elements, 3), jnp.int32),
                pltpu.VMEM((6, elements, cases), BF16),
                pltpu.VMEM((cases, 6 * elements + inner), BF16),
                pltpu.VMEM((cases, 6 * elements), BF16),
                pltpu.VMEM((fronts, 6 * elements, width), BF16),
                pltpu.VMEM((fronts, cases, width), F32),
                slots,
                pltpu.VMEM((STEPS, group, width), F32),
                slots,
                slots,
                slots,
                slots,
                dma((len(blocks),)),
                dma((2,)),
                dma((STEPS,)),
                dma((STEPS,)),
                dma((STEPS,)),
                dma((STEPS,)),
                dma((STEPS,)),
                dma((5,)),
            ],
            compiler_params=pltpu.CompilerParams(collective_id=0, has_side_effects=True),
        )(*blocks)
        return result[None]

    return jax.shard_map(
        shards,
        mesh=mesh,
        in_specs=(
            P("strip", "front", None),
            P("strip", "front", None),
            P("strip", "front", None, None),
            P("strip", "front", None, None),
            P("strip", "front", None),
            P("strip", "front", None),
            P("strip", None, "front"),
            P("strip", "front", None),
            P("strip", None, "front"),
        ),
        out_specs=P("strip", None, None, "front"),
        check_vma=False,
    )
```

```python
import functools

import jax
import jax.numpy as jnp
from jax import lax
from jax.experimental import pallas as pl
from jax.experimental.pallas import tpu as pltpu
from jax.sharding import PartitionSpec as P

MESH = pl.DeviceIdType.MESH
STEPS = 4
SIDE = 4
F32, BF16 = jnp.float32, jnp.bfloat16


def ring_gap(step):
    return min(step, SIDE - step)


def reach(k):
    return ring_gap(k // SIDE) + ring_gap(k % SIDE)


def kernel(
    strips,
    fronts,
    own_table_hbm,
    low_table_hbm,
    top_hbm,
    bottom_hbm,
    inner_hbm,
    condense_hbm,
    couple_hbm,
    inverse_hbm,
    first_hbm,
    out,
    own_table,
    low_table,
    top_loads,
    bottom_loads,
    inner_loads,
    condense,
    couple,
    inverse,
    first_front,
    own_ids,
    low_ids,
    upper,
    lhs_own,
    lhs_up,
    low_marks,
    partial,
    load_send,
    load_own,
    load_slots,
    front_slots,
    sum_send,
    sum_slots,
    sum_own,
    input_sems,
    upper_sems,
    load_sems,
    tile_sems,
    near_sems,
    far_sems,
    sum_sems,
    send_sems,
):
    strip, front = lax.axis_index("strip"), lax.axis_index("front")
    row, col = front // SIDE, front % SIDE
    group, width = first_front.shape
    cases = inner_loads.shape[1]
    peers = sorted(range(1, fronts), key=lambda k: -reach(k))
    far = [k for k in peers if reach(k) > 2]
    near = [k for k in peers if reach(k) <= 2]
    batches = [far, near[: len(near) // 2], near[len(near) // 2 :]]
    across = strip % 2

    def ahead(k):
        return ((row + k // SIDE) % SIDE) * SIDE + (col + k % SIDE) % SIDE

    def behind(k):
        return ((row + SIDE - k // SIDE) % SIDE) * SIDE + (col + SIDE - k % SIDE) % SIDE

    def panel(where):
        return pl.ds(pl.multiple_of(where * width, width), width)

    def send(src, dst, send_sem, recv_sem, where):
        pltpu.make_async_remote_copy(
            src_ref=src,
            dst_ref=dst,
            send_sem=send_sem,
            recv_sem=recv_sem,
            device_id=where,
            device_id_type=MESH,
        ).start()

    def landed(ref, sem):
        pltpu.make_async_copy(ref, ref, sem).wait()

    barrier = pltpu.get_barrier_semaphore()
    for k in peers:
        pl.semaphore_signal(barrier, 1, device_id=(strip, ahead(k)), device_id_type=MESH)

    @pl.when(strip < strips - 1)
    def _():
        pl.semaphore_signal(barrier, 1, device_id=(strip + 1, front), device_id_type=MESH)

    @pl.when(strip > 0)
    def _():
        pl.semaphore_signal(barrier, 1, device_id=(strip - 1, front), device_id_type=MESH)

    fetches = [
        pltpu.make_async_copy(src, dst, input_sems.at[i])
        for i, (src, dst) in enumerate(
            [
                (low_table_hbm, low_table),
                (own_table_hbm, own_table),
                (bottom_hbm, bottom_loads),
                (first_hbm, first_front),
                (top_hbm, top_loads),
                (inner_hbm, inner_loads),
                (condense_hbm, condense),
                (couple_hbm, couple),
                (inverse_hbm, inverse),
            ]
        )
    ]
    for copy in fetches:
        copy.start()

    def spread(table, ids):
        nodes = table[:, 0].T
        for j in range(6):
            column = 2 * nodes[:, j // 2 : j // 2 + 1] + j % 2
            ids[j] = jnp.broadcast_to(column, ids.shape[1:])

    def incidence(ids, columns):
        lanes = ids.shape[2]
        dofs = lax.broadcasted_iota(jnp.int32, ids.shape[1:], 1) + columns * width
        halves = [
            jnp.concatenate(
                [jnp.where(dofs + start == ids[j], 1.0, 0.0).astype(BF16) for j in range(6)], axis=0
            )
            for start in range(0, width, lanes)
        ]
        return jnp.concatenate(halves, axis=1)

    def turned(loads):
        return loads[...].reshape(-1, cases).astype(F32).T

    for copy in fetches[:2]:
        copy.wait()
    spread(low_table, low_ids)
    spread(own_table, own_ids)

    @pl.loop(0, fronts, unroll=4)
    def _(k):
        low_marks[k] = incidence(low_ids, ahead(k))

    for copy in fetches[2:7]:
        copy.wait()

    below = jnp.minimum(strip, 1)
    above = jnp.minimum(strips - 1 - strip, 1)
    pl.semaphore_wait(barrier, fronts - 1 + below + above)

    @pl.when(strip > 0)
    def _():
        send(bottom_loads, upper, upper_sems.at[0], upper_sems.at[1], (strip - 1, front))

    half = group // 2
    halves = [pl.ds(h * half, half) for h in (0, 1)]

    def gather_sem(step, k, h):
        return (near_sems if k in near else far_sems).at[step, h]

    for h, rows in enumerate(halves):
        for k in peers:
            send(
                first_front.at[rows],
                front_slots.at[0, k, rows],
                send_sems.at[0],
                gather_sem(0, k, h),
                (strip, ahead(k)),
            )
    front_slots[0, 0] = first_front[...]

    @pl.when(strip == 0)
    def _():
        for step in range(1, STEPS):
            front_slots[step] = jnp.zeros_like(front_slots[step])

    @pl.when(strip == strips - 1)
    def _():
        upper[...] = jnp.zeros_like(upper)

    edge_rows = 6 * top_loads.shape[1]
    lhs_own[:, :edge_rows] = turned(top_loads).astype(BF16)
    lhs_own[:, edge_rows:] = (-inner_loads[...].astype(F32).T).astype(BF16)

    @pl.loop(0, fronts, unroll=2)
    def _(k):
        where = ahead(k)
        rhs = jnp.concatenate([incidence(own_ids, where), condense[:, panel(where)]], axis=0)
        partial[k] = jnp.dot(lhs_own[...], rhs, preferred_element_type=F32)

    @pl.when(strip < strips - 1)
    def _():
        landed(upper, upper_sems.at[1])

    lhs_up[...] = turned(upper).astype(BF16)

    def loads_of(k, rows):
        return partial[k, rows] + jnp.dot(lhs_up[rows], low_marks[k], preferred_element_type=F32)

    def send_loads(step, rows, sem, ks):
        for k in ks:
            send(
                load_send.at[step, k, rows],
                load_slots.at[step, k, rows],
                send_sems.at[1],
                sem,
                (strip, ahead(k)),
            )

    for batch in batches:
        for k in batch:
            load_send[0, k] = loads_of(k, slice(0, group)).astype(BF16)
        send_loads(0, halves[0], load_sems.at[0], batch)
    send_loads(0, halves[1], load_sems.at[STEPS], peers)
    load_own[0] = loads_of(0, slice(0, group))

    @pl.loop(0, fronts, unroll=2)
    def _(k):
        rest = loads_of(k, slice(group, cases)).astype(BF16)
        for step in range(1, STEPS):
            load_send[step, k] = rest[(step - 1) * group : step * group]

    rest = loads_of(0, slice(group, cases))
    for step in range(1, STEPS):
        load_own[step] = rest[(step - 1) * group : step * group]

    for copy in fetches[7:]:
        copy.wait()

    others = pl.ds(1, fronts - 1)

    @pl.loop(0, STEPS)
    def _(step):
        @pl.when((step > 0) & (strip > 0) & (across == 0))
        def _():
            for h, rows in enumerate(halves):
                landed(front_slots.at[step, 0, rows], tile_sems.at[step, h])
                for k in peers:
                    send(
                        front_slots.at[step, 0, rows],
                        front_slots.at[step, k, rows],
                        send_sems.at[2],
                        gather_sem(step, k, h),
                        (strip, ahead(k)),
                    )

        expected = (step == 0) | (strip > 0)

        def joined_with(ks, rows):
            return functools.reduce(
                jnp.add,
                [
                    jnp.dot(
                        front_slots[step, k, rows],
                        couple[panel(behind(k)), :],
                        preferred_element_type=F32,
                    )
                    for k in ks
                ],
            )

        for h, rows in enumerate(halves):

            @pl.when(expected)
            def _():
                landed(front_slots.at[step, pl.ds(0, len(near)), rows], near_sems.at[step, h])

            @pl.when((step > 0) & (strip > 0) & (across == 1))
            def _():
                landed(front_slots.at[step, 0, rows], tile_sems.at[step, h])

            joined = joined_with([0, *near], rows)

            @pl.when(expected)
            def _():
                landed(front_slots.at[step, pl.ds(0, len(far)), rows], far_sems.at[step, h])

            joined = joined + joined_with(far, rows)

            @pl.when(step == 0)
            def _():
                landed(load_slots.at[0, others, rows], load_sems.at[0 if h == 0 else STEPS])

            if h == 0:

                @pl.when(step > 0)
                def _():
                    landed(load_slots.at[step, others], load_sems.at[step])

            total = load_own[step, rows]
            for k in peers:
                total = total + load_slots[step, k, rows].astype(F32)
            reduced = (total - joined).astype(BF16)

            def sums_for(where):
                return jnp.dot(reduced, inverse[:, panel(where)], preferred_element_type=F32)

            for batch in batches:
                for k in batch:
                    sum_send[step, k, rows] = sums_for(ahead(k)).astype(BF16)
                for k in batch:
                    send(
                        sum_send.at[step, k, rows],
                        sum_slots.at[step, k, rows],
                        send_sems.at[3],
                        sum_sems.at[step, h],
                        (strip, ahead(k)),
                    )
            sum_own[rows] = sums_for(front)

        @pl.when(step < STEPS - 1)
        def _():
            send_loads(step + 1, pl.ds(0, group), load_sems.at[step + 1], peers)

        onward = (step < STEPS - 1) & (strip < strips - 1)
        for h, rows in enumerate(halves):
            landed(sum_slots.at[step, others, rows], sum_sems.at[step, h])
            summed = sum_own[rows]
            for k in peers:
                summed = summed + sum_slots[step, k, rows].astype(F32)
            out[step, rows] = summed.astype(BF16)

            @pl.when(onward & (across == 0))
            def _():
                for k in [*far, *near, 0]:
                    send(
                        out.at[step, rows],
                        front_slots.at[step + 1, k, rows],
                        send_sems.at[4],
                        tile_sems.at[step + 1, h] if k == 0 else gather_sem(step + 1, k, h),
                        (strip + 1, ahead(k)),
                    )

            @pl.when(onward & (across == 1))
            def _():
                send(
                    out.at[step, rows],
                    front_slots.at[step + 1, 0, rows],
                    send_sems.at[4],
                    tile_sems.at[step + 1, h],
                    (strip + 1, front),
                )

    @pl.when(strip > 0)
    def _():
        landed(upper, upper_sems.at[0])

    landed(front_slots.at[0, others], send_sems.at[0])
    landed(load_slots.at[:, others], send_sems.at[1])
    landed(sum_slots.at[:, others], send_sems.at[3])

    @pl.when((strip > 0) & (across == 0))
    def _():
        landed(front_slots.at[pl.ds(1, STEPS - 1), others], send_sems.at[2])

    @pl.when((strip < strips - 1) & (across == 0))
    def _():
        landed(front_slots.at[pl.ds(1, STEPS - 1)], send_sems.at[4])

    @pl.when((strip < strips - 1) & (across == 1))
    def _():
        landed(front_slots.at[pl.ds(1, STEPS - 1), 0], send_sems.at[4])


def solution(mesh):
    strips, fronts = mesh.shape["strip"], mesh.shape["front"]

    def shards(*blocks):
        tables = [jnp.transpose(block, (2, 0, 1)) for block in blocks[:2]]
        blocks = tables + [block[0] for block in blocks[2:]]
        for i in (2, 3):
            blocks[i] = jnp.swapaxes(blocks[i], 0, 1)
        elements = blocks[2].shape[1]
        inner, cases = blocks[4].shape
        group, width = blocks[8].shape
        in_vmem = pl.BlockSpec(memory_space=pltpu.VMEM)
        in_hbm = pl.BlockSpec(memory_space=pl.ANY)
        slots = pltpu.VMEM((STEPS, fronts, group, width), BF16)
        dma = pltpu.SemaphoreType.DMA
        result = pl.pallas_call(
            functools.partial(kernel, strips, fronts),
            out_shape=jax.ShapeDtypeStruct((STEPS, group, width), BF16),
            in_specs=[in_hbm] * len(blocks),
            out_specs=in_vmem,
            scratch_shapes=[
                *[pltpu.VMEM(block.shape, block.dtype) for block in blocks],
                pltpu.VMEM((6, elements, 128), jnp.int32),
                pltpu.VMEM((6, elements, 128), jnp.int32),
                pltpu.VMEM((6, elements, cases), BF16),
                pltpu.VMEM((cases, 6 * elements + inner), BF16),
                pltpu.VMEM((cases, 6 * elements), BF16),
                pltpu.VMEM((fronts, 6 * elements, width), BF16),
                pltpu.VMEM((fronts, cases, width), F32),
                slots,
                pltpu.VMEM((STEPS, group, width), F32),
                slots,
                slots,
                slots,
                slots,
                pltpu.VMEM((group, width), F32),
                dma((len(blocks),)),
                dma((2,)),
                dma((STEPS + 1,)),
                dma((STEPS, 2)),
                dma((STEPS, 2)),
                dma((STEPS, 2)),
                dma((STEPS, 2)),
                dma((5,)),
            ],
            compiler_params=pltpu.CompilerParams(collective_id=0, has_side_effects=True),
        )(*blocks)
        return result[None]

    return jax.shard_map(
        shards,
        mesh=mesh,
        in_specs=(
            P("strip", "front", None),
            P("strip", "front", None),
            P("strip", "front", None, None),
            P("strip", "front", None, None),
            P("strip", "front", None),
            P("strip", "front", None),
            P("strip", None, "front"),
            P("strip", "front", None),
            P("strip", None, "front"),
        ),
        out_specs=P("strip", None, None, "front"),
        check_vma=False,
    )
```

```python
import functools

import jax
import jax.numpy as jnp
from jax import lax
from jax.experimental import pallas as pl
from jax.experimental.pallas import tpu as pltpu
from jax.sharding import PartitionSpec as P

MESH = pl.DeviceIdType.MESH
STEPS = 4
SIDE = 4
F32, BF16 = jnp.float32, jnp.bfloat16


def ring_gap(step):
    return min(step, SIDE - step)


def reach(k):
    return ring_gap(k // SIDE) + ring_gap(k % SIDE)


def kernel(
    strips,
    fronts,
    own_table_hbm,
    low_table_hbm,
    top_hbm,
    bottom_hbm,
    inner_hbm,
    condense_hbm,
    couple_hbm,
    inverse_hbm,
    first_hbm,
    out,
    own_table,
    low_table,
    top_loads,
    bottom_loads,
    inner_loads,
    condense,
    couple,
    inverse,
    first_front,
    own_ids,
    low_ids,
    upper,
    lhs_own,
    lhs_up,
    own_marks,
    low_marks,
    partial,
    load_send,
    load_own,
    load_slots,
    front_slots,
    sum_send,
    sum_slots,
    sum_own,
    input_sems,
    upper_sems,
    load_sems,
    tile_sems,
    near_sems,
    far_sems,
    sum_sems,
    send_sems,
):
    strip, front = lax.axis_index("strip"), lax.axis_index("front")
    row, col = front // SIDE, front % SIDE
    group, width = first_front.shape
    cases = inner_loads.shape[1]
    peers = sorted(range(1, fronts), key=lambda k: -reach(k))
    far = [k for k in peers if reach(k) > 2]
    near = [k for k in peers if reach(k) <= 2]
    batches = [far, near[: len(near) // 2], near[len(near) // 2 :]]
    across = strip % 2

    def ahead(k):
        return ((row + k // SIDE) % SIDE) * SIDE + (col + k % SIDE) % SIDE

    def behind(k):
        return ((row + SIDE - k // SIDE) % SIDE) * SIDE + (col + SIDE - k % SIDE) % SIDE

    def panel(where):
        return pl.ds(pl.multiple_of(where * width, width), width)

    def send(src, dst, send_sem, recv_sem, where):
        pltpu.make_async_remote_copy(
            src_ref=src,
            dst_ref=dst,
            send_sem=send_sem,
            recv_sem=recv_sem,
            device_id=where,
            device_id_type=MESH,
        ).start()

    def landed(ref, sem):
        pltpu.make_async_copy(ref, ref, sem).wait()

    barrier = pltpu.get_barrier_semaphore()
    for k in peers:
        pl.semaphore_signal(barrier, 1, device_id=(strip, ahead(k)), device_id_type=MESH)

    @pl.when(strip < strips - 1)
    def _():
        pl.semaphore_signal(barrier, 1, device_id=(strip + 1, front), device_id_type=MESH)

    @pl.when(strip > 0)
    def _():
        pl.semaphore_signal(barrier, 1, device_id=(strip - 1, front), device_id_type=MESH)

    fetches = [
        pltpu.make_async_copy(src, dst, input_sems.at[i])
        for i, (src, dst) in enumerate(
            [
                (low_table_hbm, low_table),
                (own_table_hbm, own_table),
                (bottom_hbm, bottom_loads),
                (first_hbm, first_front),
                (top_hbm, top_loads),
                (inner_hbm, inner_loads),
                (condense_hbm, condense),
                (couple_hbm, couple),
                (inverse_hbm, inverse),
            ]
        )
    ]
    for copy in fetches:
        copy.start()

    def products(jobs, height):
        def body(*sums):
            count = 0
            for terms, pair in zip(jobs, zip(sums[::2], sums[1::2])):
                for lhs, rhs in terms:
                    unit, stage = count % 2, count // 2 % 2
                    pltpu.matmul_push_rhs(rhs(), staging_register=stage, mxu_index=unit)
                    pltpu.matmul_acc_lhs(pair[unit], lhs(), load_staged_rhs=stage)
                    count += 1
            results, count = [], 0
            for terms, pair in zip(jobs, zip(sums[::2], sums[1::2])):
                used = sorted({(count + i) % 2 for i in range(len(terms))})
                count += len(terms)
                results.append(functools.reduce(jnp.add, [pltpu.matmul_pop(pair[unit]) for unit in used]))
            return results

        return pl.run_scoped(
            body, *[pltpu.ACC(i % 2)((height, width), F32) for i in range(2 * len(jobs))]
        )

    def spread(table, ids):
        nodes = table[:, 0].T
        for j in range(6):
            column = 2 * nodes[:, j // 2 : j // 2 + 1] + j % 2
            ids[j] = jnp.broadcast_to(column, ids.shape[1:])

    def incidence(ids, columns):
        lanes = ids.shape[2]
        dofs = lax.broadcasted_iota(jnp.int32, ids.shape[1:], 1) + columns * width
        halves = [
            jnp.concatenate(
                [jnp.where(dofs + start == ids[j], 1.0, 0.0).astype(BF16) for j in range(6)], axis=0
            )
            for start in range(0, width, lanes)
        ]
        return jnp.concatenate(halves, axis=1)

    def turned(loads):
        return loads[...].reshape(-1, cases).astype(F32).T

    for copy in fetches[:2]:
        copy.wait()
    spread(low_table, low_ids)
    spread(own_table, own_ids)

    @pl.loop(0, fronts, unroll=4)
    def _(k):
        low_marks[k, : 6 * low_ids.shape[1]] = incidence(low_ids, ahead(k))
        low_marks[k, 6 * low_ids.shape[1] :] = jnp.zeros((2 * width - 6 * low_ids.shape[1], width), BF16)

    for copy in fetches[2:7]:
        copy.wait()

    below = jnp.minimum(strip, 1)
    above = jnp.minimum(strips - 1 - strip, 1)
    pl.semaphore_wait(barrier, fronts - 1 + below + above)

    @pl.when(strip > 0)
    def _():
        send(bottom_loads, upper, upper_sems.at[0], upper_sems.at[1], (strip - 1, front))

    half = group // 2
    halves = [pl.ds(h * half, half) for h in (0, 1)]

    def gather_sem(step, k, h):
        return (near_sems if k in near else far_sems).at[step, h]

    for h, rows in enumerate(halves):
        for k in peers:
            send(
                first_front.at[rows],
                front_slots.at[0, k, rows],
                send_sems.at[0],
                gather_sem(0, k, h),
                (strip, ahead(k)),
            )
    front_slots[0, 0] = first_front[...]

    @pl.when(strip == 0)
    def _():
        for step in range(1, STEPS):
            front_slots[step] = jnp.zeros_like(front_slots[step])

    @pl.when(strip == strips - 1)
    def _():
        upper[...] = jnp.zeros_like(upper)

    edge_rows = 6 * top_loads.shape[1]
    inner_rows = inner_loads.shape[0]
    lhs_own[...] = jnp.zeros_like(lhs_own)
    lhs_own[:, :edge_rows] = turned(top_loads).astype(BF16)
    lhs_own[:, edge_rows : edge_rows + inner_rows] = (-inner_loads[...].astype(F32).T).astype(BF16)
    own_marks[...] = jnp.zeros_like(own_marks)

    @pl.loop(0, fronts, unroll=2)
    def _(k):
        where, slot = ahead(k), k % 2
        own_marks[slot, :edge_rows] = incidence(own_ids, where)
        own_marks[slot, edge_rows : edge_rows + inner_rows] = condense[:, panel(where)]
        terms = [
            (
                lambda at=at: lhs_own[:, at],
                lambda at=at: own_marks[slot, at],
            )
            for at in (slice(0, width), slice(width, 2 * width))
        ]
        partial[k] = products([terms], cases)[0]

    @pl.when(strip < strips - 1)
    def _():
        landed(upper, upper_sems.at[1])

    lhs_up[...] = jnp.zeros_like(lhs_up)
    lhs_up[:, :edge_rows] = turned(upper).astype(BF16)

    def loads_of(ks, rows):
        jobs = [
            [
                (
                    lambda at=at: lhs_up[rows, at],
                    lambda at=at, k=k: low_marks[k, at],
                )
                for at in (slice(0, width), slice(width, 2 * width))
            ]
            for k in ks
        ]
        return [
            partial[k, rows] + result
            for k, result in zip(ks, products(jobs, rows.stop - rows.start))
        ]

    def send_loads(step, rows, sem, ks):
        for k in ks:
            send(
                load_send.at[step, k, rows],
                load_slots.at[step, k, rows],
                send_sems.at[1],
                sem,
                (strip, ahead(k)),
            )

    for batch in batches:
        for k, result in zip(batch, loads_of(batch, slice(0, group))):
            load_send[0, k] = result.astype(BF16)
        send_loads(0, halves[0], load_sems.at[0], batch)
    send_loads(0, halves[1], load_sems.at[STEPS], peers)
    load_own[0] = loads_of([0], slice(0, group))[0]

    @pl.loop(0, fronts, unroll=2)
    def _(k):
        rest = loads_of([k], slice(group, cases))[0].astype(BF16)
        for step in range(1, STEPS):
            load_send[step, k] = rest[(step - 1) * group : step * group]

    rest = loads_of([0], slice(group, cases))[0]
    for step in range(1, STEPS):
        load_own[step] = rest[(step - 1) * group : step * group]

    send_loads(1, pl.ds(0, group), load_sems.at[1], peers)

    for copy in fetches[7:]:
        copy.wait()

    others = pl.ds(1, fronts - 1)

    @pl.loop(0, STEPS)
    def _(step):
        @pl.when((step > 0) & (strip > 0) & (across == 0))
        def _():
            for h, rows in enumerate(halves):
                landed(front_slots.at[step, 0, rows], tile_sems.at[step, h])
                for k in peers:
                    send(
                        front_slots.at[step, 0, rows],
                        front_slots.at[step, k, rows],
                        send_sems.at[2],
                        gather_sem(step, k, h),
                        (strip, ahead(k)),
                    )

        expected = (step == 0) | (strip > 0)

        def joined_with(ks, rows):
            terms = [
                (
                    lambda k=k: front_slots[step, k, rows],
                    lambda k=k: couple[panel(behind(k)), :],
                )
                for k in ks
            ]
            return products([terms], half)[0]

        for h, rows in enumerate(halves):

            @pl.when(expected)
            def _():
                landed(front_slots.at[step, pl.ds(0, len(near)), rows], near_sems.at[step, h])

            @pl.when((step > 0) & (strip > 0) & (across == 1))
            def _():
                landed(front_slots.at[step, 0, rows], tile_sems.at[step, h])

            joined = joined_with([0, *near], rows)

            @pl.when(expected)
            def _():
                landed(front_slots.at[step, pl.ds(0, len(far)), rows], far_sems.at[step, h])

            joined = joined + joined_with(far, rows)

            @pl.when(step == 0)
            def _():
                landed(load_slots.at[0, others, rows], load_sems.at[0 if h == 0 else STEPS])

            if h == 0:

                @pl.when(step > 0)
                def _():
                    landed(load_slots.at[step, others], load_sems.at[step])

            total = load_own[step, rows]
            for k in peers:
                total = total + load_slots[step, k, rows].astype(F32)
            reduced = (total - joined).astype(BF16)

            for batch in batches:
                wheres = [ahead(k) for k in batch] + ([front] if batch is batches[-1] else [])
                jobs = [[(lambda: reduced, lambda w=w: inverse[:, panel(w)])] for w in wheres]
                results = products(jobs, half)
                for k, result in zip(batch, results):
                    sum_send[step, k, rows] = result.astype(BF16)
                for k in batch:
                    send(
                        sum_send.at[step, k, rows],
                        sum_slots.at[step, k, rows],
                        send_sems.at[3],
                        sum_sems.at[step, h],
                        (strip, ahead(k)),
                    )
            sum_own[rows] = results[-1]

        @pl.when(step < STEPS - 2)
        def _():
            send_loads(step + 2, pl.ds(0, group), load_sems.at[step + 2], peers)

        onward = (step < STEPS - 1) & (strip < strips - 1)
        for h, rows in enumerate(halves):
            landed(sum_slots.at[step, others, rows], sum_sems.at[step, h])
            summed = sum_own[rows]
            for k in peers:
                summed = summed + sum_slots[step, k, rows].astype(F32)
            out[step, rows] = summed.astype(BF16)

            @pl.when(onward & (across == 0))
            def _():
                for k in [*far, *near, 0]:
                    send(
                        out.at[step, rows],
                        front_slots.at[step + 1, k, rows],
                        send_sems.at[4],
                        tile_sems.at[step + 1, h] if k == 0 else gather_sem(step + 1, k, h),
                        (strip + 1, ahead(k)),
                    )

            @pl.when(onward & (across == 1))
            def _():
                send(
                    out.at[step, rows],
                    front_slots.at[step + 1, 0, rows],
                    send_sems.at[4],
                    tile_sems.at[step + 1, h],
                    (strip + 1, front),
                )

    @pl.when(strip > 0)
    def _():
        landed(upper, upper_sems.at[0])

    landed(front_slots.at[0, others], send_sems.at[0])
    landed(load_slots.at[:, others], send_sems.at[1])
    landed(sum_slots.at[:, others], send_sems.at[3])

    @pl.when((strip > 0) & (across == 0))
    def _():
        landed(front_slots.at[pl.ds(1, STEPS - 1), others], send_sems.at[2])

    @pl.when((strip < strips - 1) & (across == 0))
    def _():
        landed(front_slots.at[pl.ds(1, STEPS - 1)], send_sems.at[4])

    @pl.when((strip < strips - 1) & (across == 1))
    def _():
        landed(front_slots.at[pl.ds(1, STEPS - 1), 0], send_sems.at[4])


def solution(mesh):
    strips, fronts = mesh.shape["strip"], mesh.shape["front"]

    def shards(*blocks):
        tables = [jnp.transpose(block, (2, 0, 1)) for block in blocks[:2]]
        blocks = tables + [block[0] for block in blocks[2:]]
        for i in (2, 3):
            blocks[i] = jnp.swapaxes(blocks[i], 0, 1)
        elements = blocks[2].shape[1]
        inner, cases = blocks[4].shape
        group, width = blocks[8].shape
        in_vmem = pl.BlockSpec(memory_space=pltpu.VMEM)
        in_hbm = pl.BlockSpec(memory_space=pl.ANY)
        slots = pltpu.VMEM((STEPS, fronts, group, width), BF16)
        dma = pltpu.SemaphoreType.DMA
        result = pl.pallas_call(
            functools.partial(kernel, strips, fronts),
            out_shape=jax.ShapeDtypeStruct((STEPS, group, width), BF16),
            in_specs=[in_hbm] * len(blocks),
            out_specs=in_vmem,
            scratch_shapes=[
                *[pltpu.VMEM(block.shape, block.dtype) for block in blocks],
                pltpu.VMEM((6, elements, 128), jnp.int32),
                pltpu.VMEM((6, elements, 128), jnp.int32),
                pltpu.VMEM((6, elements, cases), BF16),
                pltpu.VMEM((cases, 2 * width), BF16),
                pltpu.VMEM((cases, 2 * width), BF16),
                pltpu.VMEM((2, 2 * width, width), BF16),
                pltpu.VMEM((fronts, 2 * width, width), BF16),
                pltpu.VMEM((fronts, cases, width), F32),
                slots,
                pltpu.VMEM((STEPS, group, width), F32),
                slots,
                slots,
                slots,
                slots,
                pltpu.VMEM((group, width), F32),
                dma((len(blocks),)),
                dma((2,)),
                dma((STEPS + 1,)),
                dma((STEPS, 2)),
                dma((STEPS, 2)),
                dma((STEPS, 2)),
                dma((STEPS, 2)),
                dma((5,)),
            ],
            compiler_params=pltpu.CompilerParams(collective_id=0, has_side_effects=True),
        )(*blocks)
        return result[None]

    return jax.shard_map(
        shards,
        mesh=mesh,
        in_specs=(
            P("strip", "front", None),
            P("strip", "front", None),
            P("strip", "front", None, None),
            P("strip", "front", None, None),
            P("strip", "front", None),
            P("strip", "front", None),
            P("strip", None, "front"),
            P("strip", "front", None),
            P("strip", None, "front"),
        ),
        out_specs=P("strip", None, None, "front"),
        check_vma=False,
    )
```

```python
import functools

import jax
import jax.numpy as jnp
from jax import lax
from jax.experimental import pallas as pl
from jax.experimental.pallas import tpu as pltpu
from jax.sharding import PartitionSpec as P

MESH = pl.DeviceIdType.MESH
STEPS = 4
SIDE = 4
F32, BF16 = jnp.float32, jnp.bfloat16


def ring_gap(step):
    return min(step, SIDE - step)


def reach(k):
    return ring_gap(k // SIDE) + ring_gap(k % SIDE)


def kernel(
    strips,
    fronts,
    own_table_hbm,
    low_table_hbm,
    top_hbm,
    bottom_hbm,
    inner_hbm,
    condense_hbm,
    couple_hbm,
    inverse_hbm,
    first_hbm,
    out,
    own_table,
    low_table,
    top_loads,
    bottom_loads,
    inner_loads,
    condense,
    couple,
    inverse,
    first_front,
    own_ids,
    low_ids,
    upper,
    lhs_own,
    lhs_up,
    own_marks,
    low_marks,
    partial,
    load_send,
    load_own,
    load_slots,
    front_slots,
    sum_send,
    sum_slots,
    sum_own,
    input_sems,
    upper_sems,
    load_sems,
    tile_sems,
    near_sems,
    far_sems,
    sum_sems,
    send_sems,
):
    strip, front = lax.axis_index("strip"), lax.axis_index("front")
    row, col = front // SIDE, front % SIDE
    group, width = first_front.shape
    cases = inner_loads.shape[1]
    peers = sorted(range(1, fronts), key=lambda k: -reach(k))
    far = [k for k in peers if reach(k) > 2]
    near = [k for k in peers if reach(k) <= 2]
    batches = [far, near[: len(near) // 2], near[len(near) // 2 :]]

    def ahead(k):
        return ((row + k // SIDE) % SIDE) * SIDE + (col + k % SIDE) % SIDE

    def behind(k):
        return ((row + SIDE - k // SIDE) % SIDE) * SIDE + (col + SIDE - k % SIDE) % SIDE

    def panel(where):
        return pl.ds(pl.multiple_of(where * width, width), width)

    def send(src, dst, send_sem, recv_sem, where):
        pltpu.make_async_remote_copy(
            src_ref=src,
            dst_ref=dst,
            send_sem=send_sem,
            recv_sem=recv_sem,
            device_id=where,
            device_id_type=MESH,
        ).start()

    def landed(ref, sem):
        pltpu.make_async_copy(ref, ref, sem).wait()

    barrier = pltpu.get_barrier_semaphore()
    for k in peers:
        pl.semaphore_signal(barrier, 1, device_id=(strip, ahead(k)), device_id_type=MESH)

    @pl.when(strip < strips - 1)
    def _():
        pl.semaphore_signal(barrier, 1, device_id=(strip + 1, front), device_id_type=MESH)

    @pl.when(strip > 0)
    def _():
        pl.semaphore_signal(barrier, 1, device_id=(strip - 1, front), device_id_type=MESH)

    fetches = [
        pltpu.make_async_copy(src, dst, input_sems.at[i])
        for i, (src, dst) in enumerate(
            [
                (low_table_hbm, low_table),
                (own_table_hbm, own_table),
                (bottom_hbm, bottom_loads),
                (first_hbm, first_front),
                (top_hbm, top_loads),
                (inner_hbm, inner_loads),
                (condense_hbm, condense),
                (couple_hbm, couple),
                (inverse_hbm, inverse),
            ]
        )
    ]
    for copy in fetches:
        copy.start()

    def products(jobs, height):
        def body(*sums):
            count = 0
            for terms, pair in zip(jobs, zip(sums[::2], sums[1::2])):
                for lhs, rhs in terms:
                    unit, stage = count % 2, count // 2 % 2
                    pltpu.matmul_push_rhs(rhs(), staging_register=stage, mxu_index=unit)
                    pltpu.matmul_acc_lhs(pair[unit], lhs(), load_staged_rhs=stage)
                    count += 1
            results, count = [], 0
            for terms, pair in zip(jobs, zip(sums[::2], sums[1::2])):
                used = sorted({(count + i) % 2 for i in range(len(terms))})
                count += len(terms)
                results.append(functools.reduce(jnp.add, [pltpu.matmul_pop(pair[unit]) for unit in used]))
            return results

        return pl.run_scoped(
            body, *[pltpu.ACC(i % 2)((height, width), F32) for i in range(2 * len(jobs))]
        )

    def spread(table, ids):
        nodes = table[:, 0].T
        for j in range(6):
            column = 2 * nodes[:, j // 2 : j // 2 + 1] + j % 2
            ids[j] = jnp.broadcast_to(column, ids.shape[1:])

    def incidence(ids, columns):
        lanes = ids.shape[2]
        dofs = lax.broadcasted_iota(jnp.int32, ids.shape[1:], 1) + columns * width
        halves = [
            jnp.concatenate(
                [jnp.where(dofs + start == ids[j], 1.0, 0.0).astype(BF16) for j in range(6)], axis=0
            )
            for start in range(0, width, lanes)
        ]
        return jnp.concatenate(halves, axis=1)

    def turned(loads):
        return loads[...].reshape(-1, cases).astype(F32).T

    for copy in fetches[:2]:
        copy.wait()
    spread(low_table, low_ids)
    spread(own_table, own_ids)

    @pl.loop(0, fronts, unroll=4)
    def _(k):
        low_marks[k, : 6 * low_ids.shape[1]] = incidence(low_ids, ahead(k))
        low_marks[k, 6 * low_ids.shape[1] :] = jnp.zeros((2 * width - 6 * low_ids.shape[1], width), BF16)

    for copy in fetches[2:7]:
        copy.wait()

    below = jnp.minimum(strip, 1)
    above = jnp.minimum(strips - 1 - strip, 1)
    pl.semaphore_wait(barrier, fronts - 1 + below + above)

    @pl.when(strip > 0)
    def _():
        send(bottom_loads, upper, upper_sems.at[0], upper_sems.at[1], (strip - 1, front))

    half = group // 2
    halves = [pl.ds(h * half, half) for h in (0, 1)]

    def gather_sem(step, k, h):
        return (near_sems if k in near else far_sems).at[step, h]

    for h, rows in enumerate(halves):
        for k in peers:
            send(
                first_front.at[rows],
                front_slots.at[0, k, rows],
                send_sems.at[0],
                gather_sem(0, k, h),
                (strip, ahead(k)),
            )
    front_slots[0, 0] = first_front[...]

    @pl.when(strip == 0)
    def _():
        for step in range(1, STEPS):
            front_slots[step] = jnp.zeros_like(front_slots[step])

    @pl.when(strip == strips - 1)
    def _():
        upper[...] = jnp.zeros_like(upper)

    edge_rows = 6 * top_loads.shape[1]
    inner_rows = inner_loads.shape[0]
    lhs_own[...] = jnp.zeros_like(lhs_own)
    lhs_own[:, :edge_rows] = turned(top_loads).astype(BF16)
    lhs_own[:, edge_rows : edge_rows + inner_rows] = (-inner_loads[...].astype(F32).T).astype(BF16)
    own_marks[...] = jnp.zeros_like(own_marks)

    @pl.loop(0, fronts, unroll=2)
    def _(k):
        where, slot = ahead(k), k % 2
        own_marks[slot, :edge_rows] = incidence(own_ids, where)
        own_marks[slot, edge_rows : edge_rows + inner_rows] = condense[:, panel(where)]
        terms = [
            (
                lambda at=at: lhs_own[:, at],
                lambda at=at: own_marks[slot, at],
            )
            for at in (slice(0, width), slice(width, 2 * width))
        ]
        partial[k] = products([terms], cases)[0]

    @pl.when(strip < strips - 1)
    def _():
        landed(upper, upper_sems.at[1])

    lhs_up[...] = jnp.zeros_like(lhs_up)
    lhs_up[:, :edge_rows] = turned(upper).astype(BF16)

    def loads_of(ks, rows):
        jobs = [
            [
                (
                    lambda at=at: lhs_up[rows, at],
                    lambda at=at, k=k: low_marks[k, at],
                )
                for at in (slice(0, width), slice(width, 2 * width))
            ]
            for k in ks
        ]
        return [
            partial[k, rows] + result
            for k, result in zip(ks, products(jobs, rows.stop - rows.start))
        ]

    def send_loads(step, rows, sem, ks):
        for k in ks:
            send(
                load_send.at[step, k, rows],
                load_slots.at[step, k, rows],
                send_sems.at[1],
                sem,
                (strip, ahead(k)),
            )

    for batch in batches:
        for k, result in zip(batch, loads_of(batch, slice(0, group))):
            load_send[0, k] = result.astype(BF16)
        send_loads(0, halves[0], load_sems.at[0], batch)
    send_loads(0, halves[1], load_sems.at[STEPS], peers)
    load_own[0] = loads_of([0], slice(0, group))[0]

    @pl.loop(0, fronts, unroll=2)
    def _(k):
        rest = loads_of([k], slice(group, cases))[0].astype(BF16)
        for step in range(1, STEPS):
            load_send[step, k] = rest[(step - 1) * group : step * group]

    rest = loads_of([0], slice(group, cases))[0]
    for step in range(1, STEPS):
        load_own[step] = rest[(step - 1) * group : step * group]

    send_loads(1, pl.ds(0, group), load_sems.at[1], peers)

    for copy in fetches[7:]:
        copy.wait()

    others = pl.ds(1, fronts - 1)

    @pl.loop(0, STEPS)
    def _(step):
        expected = (step == 0) | (strip > 0)

        def joined_with(ks, rows):
            terms = [
                (
                    lambda k=k: front_slots[step, k, rows],
                    lambda k=k: couple[panel(behind(k)), :],
                )
                for k in ks
            ]
            return products([terms], half)[0]

        for h, rows in enumerate(halves):

            @pl.when(expected)
            def _():
                landed(front_slots.at[step, pl.ds(0, len(near)), rows], near_sems.at[step, h])

            @pl.when((step > 0) & (strip > 0))
            def _():
                landed(front_slots.at[step, 0, rows], tile_sems.at[step, h])

            joined = joined_with([0, *near], rows)

            @pl.when(expected)
            def _():
                landed(front_slots.at[step, pl.ds(0, len(far)), rows], far_sems.at[step, h])

            joined = joined + joined_with(far, rows)

            @pl.when(step == 0)
            def _():
                landed(load_slots.at[0, others, rows], load_sems.at[0 if h == 0 else STEPS])

            if h == 0:

                @pl.when(step > 0)
                def _():
                    landed(load_slots.at[step, others], load_sems.at[step])

            total = load_own[step, rows]
            for k in peers:
                total = total + load_slots[step, k, rows].astype(F32)
            reduced = (total - joined).astype(BF16)

            for batch in batches:
                wheres = [ahead(k) for k in batch] + ([front] if batch is batches[-1] else [])
                jobs = [[(lambda: reduced, lambda w=w: inverse[:, panel(w)])] for w in wheres]
                results = products(jobs, half)
                for k, result in zip(batch, results):
                    sum_send[step, k, rows] = result.astype(BF16)
                for k in batch:
                    send(
                        sum_send.at[step, k, rows],
                        sum_slots.at[step, k, rows],
                        send_sems.at[3],
                        sum_sems.at[step, h],
                        (strip, ahead(k)),
                    )
            sum_own[rows] = results[-1]

        @pl.when(step < STEPS - 2)
        def _():
            send_loads(step + 2, pl.ds(0, group), load_sems.at[step + 2], peers)

        onward = (step < STEPS - 1) & (strip < strips - 1)
        for h, rows in enumerate(halves):
            landed(sum_slots.at[step, others, rows], sum_sems.at[step, h])
            summed = sum_own[rows]
            for k in peers:
                summed = summed + sum_slots[step, k, rows].astype(F32)
            out[step, rows] = summed.astype(BF16)

            @pl.when(onward)
            def _():
                for k in [*far, *near, 0]:
                    send(
                        out.at[step, rows],
                        front_slots.at[step + 1, k, rows],
                        send_sems.at[4],
                        tile_sems.at[step + 1, h] if k == 0 else gather_sem(step + 1, k, h),
                        (strip + 1, ahead(k)),
                    )

    @pl.when(strip > 0)
    def _():
        landed(upper, upper_sems.at[0])

    landed(front_slots.at[0, others], send_sems.at[0])
    landed(load_slots.at[:, others], send_sems.at[1])
    landed(sum_slots.at[:, others], send_sems.at[3])

    @pl.when(strip < strips - 1)
    def _():
        landed(front_slots.at[pl.ds(1, STEPS - 1)], send_sems.at[4])


def solution(mesh):
    strips, fronts = mesh.shape["strip"], mesh.shape["front"]

    def shards(*blocks):
        tables = [jnp.transpose(block, (2, 0, 1)) for block in blocks[:2]]
        blocks = tables + [block[0] for block in blocks[2:]]
        for i in (2, 3):
            blocks[i] = jnp.swapaxes(blocks[i], 0, 1)
        elements = blocks[2].shape[1]
        inner, cases = blocks[4].shape
        group, width = blocks[8].shape
        in_vmem = pl.BlockSpec(memory_space=pltpu.VMEM)
        in_hbm = pl.BlockSpec(memory_space=pl.ANY)
        slots = pltpu.VMEM((STEPS, fronts, group, width), BF16)
        dma = pltpu.SemaphoreType.DMA
        result = pl.pallas_call(
            functools.partial(kernel, strips, fronts),
            out_shape=jax.ShapeDtypeStruct((STEPS, group, width), BF16),
            in_specs=[in_hbm] * len(blocks),
            out_specs=in_vmem,
            scratch_shapes=[
                *[pltpu.VMEM(block.shape, block.dtype) for block in blocks],
                pltpu.VMEM((6, elements, 128), jnp.int32),
                pltpu.VMEM((6, elements, 128), jnp.int32),
                pltpu.VMEM((6, elements, cases), BF16),
                pltpu.VMEM((cases, 2 * width), BF16),
                pltpu.VMEM((cases, 2 * width), BF16),
                pltpu.VMEM((2, 2 * width, width), BF16),
                pltpu.VMEM((fronts, 2 * width, width), BF16),
                pltpu.VMEM((fronts, cases, width), F32),
                slots,
                pltpu.VMEM((STEPS, group, width), F32),
                slots,
                slots,
                slots,
                slots,
                pltpu.VMEM((group, width), F32),
                dma((len(blocks),)),
                dma((2,)),
                dma((STEPS + 1,)),
                dma((STEPS, 2)),
                dma((STEPS, 2)),
                dma((STEPS, 2)),
                dma((STEPS, 2)),
                dma((5,)),
            ],
            compiler_params=pltpu.CompilerParams(collective_id=0, has_side_effects=True),
        )(*blocks)
        return result[None]

    return jax.shard_map(
        shards,
        mesh=mesh,
        in_specs=(
            P("strip", "front", None),
            P("strip", "front", None),
            P("strip", "front", None, None),
            P("strip", "front", None, None),
            P("strip", "front", None),
            P("strip", "front", None),
            P("strip", None, "front"),
            P("strip", "front", None),
            P("strip", None, "front"),
        ),
        out_specs=P("strip", None, None, "front"),
        check_vma=False,
    )
```
